256 devices in a mesh: dp: 32 (over z, x_hi, core), mp: 8 (over x_lo, y).
Axes of the slice: x: 4 (x_hi: 2, x_lo: 2; x = x_hi * 2 + x_lo), y: 4, z: 8, core: 2. Of those that a mesh axis runs over, the one named last changes fastest.
Arguments:
- tokens: bfloat16 [1024, 16384], P('dp', 'mp'), may hold values from -6 to 6
- gate_weight: bfloat16 [16384, 28672], P('mp', 'dp'), may hold values from -0.046875 to 0.046875
- up_weight: bfloat16 [16384, 28672], P('mp', 'dp'), may hold values from -0.046875 to 0.046875
- down_weight: bfloat16 [28672, 16384], P('dp', 'mp'), may hold values from -0.03125 to 0.03125
Outputs:
- mixed: bfloat16 [1024, 16384], P('dp', 'mp')
The draws below stay inside these ranges and needn't reach their ends.
All inputs are finite; a program needn't handle non-finite values.
Results may differ from the reference program's by a relative error of at most 0.0049.
Values may be sent and summed in bfloat16 or wider, within the bound.
A program may use at most 64 MiB of HBM per device.

```python
import jax
import jax.numpy as jnp

D = 16384
FF = 28672
TOKENS = 1024


def block_scale(own_key, dims, pieces, low, largest):
    def one(position, blocks):
        heights = jax.random.uniform(jax.random.fold_in(jax.random.fold_in(own_key, 6), position), (blocks,), jnp.float32, low / len(pieces), largest / len(pieces))
        return jnp.repeat(jnp.exp(heights), dims[position] // blocks).reshape((-1,) + (1,) * (len(dims) - position - 1))

    gain = one(*pieces[0])
    for cut in pieces[1:]:
        gain = gain * one(*cut)
    return gain


def noise(own_key, shape, width, most, cuts=(), held_as=jnp.bfloat16):
    drawn = jax.random.normal(own_key, shape, jnp.float32) * width
    if len(cuts) > 0:
        drawn = block_scale(own_key, shape, cuts, -0.22, 0.18) * drawn
    return jnp.clip(drawn, min=-most, max=most).astype(held_as)


def setup_inputs(seed: int = 0) -> dict:
    splits = jax.random.split(jax.random.key(seed), 5)
    tokens = noise(splits[0], (TOKENS, D), 1.0, 6.0, ((0, 32), (1, 8)))
    gate_weight = noise(splits[1], (D, FF), D ** -0.5, 0.046875, ((0, 8), (1, 32)))
    up_weight = noise(splits[2], (D, FF), D ** -0.5, 0.046875, ((0, 8), (1, 32)))
    down_weight = noise(splits[3], (FF, D), FF ** -0.5, 0.03125, ((0, 32), (1, 8)))
    return dict(tokens=tokens, gate_weight=gate_weight, up_weight=up_weight, down_weight=down_weight)


def reference(tokens, gate_weight, up_weight, down_weight):
    gate = jnp.dot(tokens, gate_weight, preferred_element_type=jnp.float32)
    up = jnp.dot(tokens, up_weight, preferred_element_type=jnp.float32)
    hidden = (jax.nn.silu(gate) * up).astype(jnp.bfloat16)
    return jnp.dot(hidden, down_weight, preferred_element_type=jnp.float32).astype(jnp.bfloat16)
```

```python
import jax
import jax.numpy as jnp
from jax import lax
from jax.experimental import pallas as pl
from jax.experimental.pallas import tpu as pltpu
from jax.sharding import PartitionSpec as P

MESH = pl.DeviceIdType.MESH
BF16, F32 = jnp.bfloat16, jnp.float32
SLABS = 8
PLAN = (
    ("gate_up", 1),
    ("add_y", 2),
    ("spread_y", 3),
    ("down", 4),
    ("send_z", 5),
    ("relay_y", 1),
    ("activate", 2),
    ("to_twin", 3),
)
HOP_TICKS = (0, 1, 3, 4, 5)

COPIES = dict(
    pair=1, up_ring=4, down_ring=4, twin_in=8,
    far=16, direct=16, joint=16, cross=8, cross_h=8, spread=24, twin_h=8,
    half=8, home=8, out=1, weight=1,
)
BASE, TOTAL = {}, 0
for _name, _count in COPIES.items():
    BASE[_name], TOTAL = TOTAL, TOTAL + _count


def kernel(tokens, gate_w, up_w, down_w, out, T, GU, DW, PG, FS, FR, SS, SR, YB, XR, HB, PO, XS, XD, ZS, ZR, FIN, OS, OR, local, sent, got):
    dp, mp = lax.axis_index("dp"), lax.axis_index("mp")
    z, xh, c = dp // 4, (dp // 2) & 1, dp & 1
    xl, y = mp // 4, mp & 3
    width = gate_w.shape[1]
    half = DW.shape[2]

    def device(z_=z, xh_=xh, c_=c, xl_=xl, y_=y):
        return (z_ * 4 + xh_ * 2 + c_, xl_ * 4 + y_)

    twin = device(c_=1 - c)
    pair = device(xh_=1 - xh)
    cross = device(xl_=1 - xl)
    y_up, y_down, y_far = (device(y_=(y + n) & 3) for n in (1, 3, 2))

    def at_z(n):
        return device(z_=(z + n) & 7)

    mine = pl.multiple_of(c * half, half)
    other = pl.multiple_of((1 - c) * half, half)
    loads = [
        pltpu.make_async_copy(tokens, T.at[z, 2 * c + xh], local.at[0]),
        pltpu.make_async_copy(gate_w, GU.at[:, pl.ds(0, width)], local.at[1]),
        pltpu.make_async_copy(up_w, GU.at[:, pl.ds(width, width)], local.at[2]),
        pltpu.make_async_copy(down_w.at[:, pl.ds(mine, half)], DW.at[c], local.at[3]),
    ]
    for load in loads:
        load.start()

    barrier = pltpu.get_barrier_semaphore()
    friends = [twin, pair, cross, y_up, y_down, y_far] + [at_z(n) for n in range(1, 8)]
    for friend in friends:
        pl.semaphore_signal(barrier, inc=1, device_id=friend, device_id_type=MESH)
    pl.semaphore_wait(barrier, len(friends))

    def copy(name, n, src, dst, to, lands=None):
        return pltpu.make_async_remote_copy(
            src_ref=src,
            dst_ref=dst,
            send_sem=sent.at[BASE[name] + n],
            recv_sem=got.at[BASE[name] + (n if lands is None else lands)],
            device_id=to,
            device_id_type=MESH,
        )

    def slab(n):
        return (z + n) & 7

    def ring_piece(n):
        return T.at[slab(n), pl.ds(2 * c, 2)]

    def ring_half(n, side):
        return T.at[slab(n), pl.ds(2 * c, 2), :, pl.ds(side * half, half)]

    def ring_down(hop):
        ref = ring_piece(hop) if hop < 3 else ring_half(hop, 0)
        return copy("down_ring", hop, ref, ref, at_z(7))

    def ring_up(hop):
        ref = ring_piece(-hop) if hop < 3 else ring_half(-hop, 1)
        return copy("up_ring", hop, ref, ref, at_z(1))

    def from_above(hop):
        ref = ring_piece(hop + 1) if hop < 3 else ring_half(hop + 1, 0)
        return copy("down_ring", hop, ref, ref, at_z(1))

    def from_below(hop):
        ref = ring_piece(-hop - 1) if hop < 3 else ring_half(-hop - 1, 1)
        return copy("up_ring", hop, ref, ref, at_z(7))

    def twin_in(n, core):
        ref = T.at[slab(n), pl.ds(2 * core, 2)]
        return copy("twin_in", n & 7, ref, ref, twin)

    def pair_in(half_):
        ref = T.at[z, 2 * c + half_]
        return copy("pair", 0, ref, ref, pair)

    weight_out = copy("weight", 0, down_w.at[:, pl.ds(other, half)], DW.at[c], twin)
    weight_in = copy("weight", 0, DW.at[1 - c], DW.at[1 - c], twin)

    def hop(n):
        if n == 0:
            loads[0].wait()
            pair_in(xh).start()
            pair_in(1 - xh).wait_recv()
            ring_down(0).start()
            ring_up(0).start()
            twin_in(0, c).start()
            weight_out.start()
            return
        from_above(n - 1).wait_recv()
        from_below(n - 1).wait_recv()
        if n < 4:
            ring_down(n).start()
            ring_up(n).start()
            twin_in(n, c).start()
            twin_in(-n, c).start()
        else:
            twin_in(4, c).start()

    def place(k):
        return jnp.where(k == 2, 7, jnp.where(k < 2, k, k - 1))

    def far(k, g):
        return copy("far", 2 * k + g, FS.at[k, g], FR.at[k, g], y_down if g else y_up)

    def joint(k, g):
        return copy("joint", 2 * k + g, SS.at[k, g], SR.at[k, g], y_down if g else y_up)

    def direct(k, g):
        return copy("direct", 2 * k + g, SS.at[k, 2 + g], SR.at[k, 2 + g], y_up if g else y_down)

    def cross_sum(k):
        return copy("cross", k, YB.at[k, 1 - xl], XR.at[k], cross)

    def cross_h(k, x):
        ref = HB.at[k, c, y, x]
        return copy("cross_h", k, ref, ref, cross)

    def spread(k, n, row, to):
        ref = HB.at[k, c, row]
        return copy("spread", 3 * k + n, ref, ref, to)

    def spreads(k):
        return [spread(k, n, y, to) for n, to in enumerate((y_up, y_down, y_far))]

    def spread_in(k):
        return [spread(k, n, (y + m) & 3, y_far) for n, m in enumerate((3, 1, 2))]

    def twin_h(k, core):
        ref = HB.at[k, core]
        return copy("twin_h", k, ref, ref, twin)

    def halves(k):
        return copy("half", k, XS.at[k], XD.at[k], pair)

    def home(k):
        return copy("home", k, ZS.at[k], ZR.at[k], at_z(place(k)))

    def gate_up(k):
        n = place(k)
        s = slab(n)
        twin_in(n, 1 - c).wait_recv()

        @pl.when(k == 0)
        def _():
            loads[1].wait()
            loads[2].wait()

        @pl.loop(0, 7)
        def _(i):
            columns = pl.ds(pl.multiple_of(i * 256, 256), 256)
            rows = jnp.concatenate([T[s, (y + m) & 3] for m in (2, 1, 3, 0)], axis=0)
            PG[k, :, columns] = jnp.dot(rows, GU[:, columns], preferred_element_type=F32)

        FS[k, 0] = PG[k, 0:32, 0:width].astype(BF16)
        FS[k, 1] = PG[k, 0:32, width:].astype(BF16)
        far(k, 0).start()
        far(k, 1).start()
        SS[k, 2] = PG[k, 64:96, 0:width].astype(BF16)
        SS[k, 3] = PG[k, 32:64, width:].astype(BF16)
        direct(k, 0).start()
        direct(k, 1).start()

    def relay_y(k):
        far(k, 0).wait_recv()
        far(k, 1).wait_recv()
        SS[k, 0] = (PG[k, 32:64, 0:width] + FR[k, 0].astype(F32)).astype(BF16)
        SS[k, 1] = (PG[k, 64:96, width:] + FR[k, 1].astype(F32)).astype(BF16)
        joint(k, 0).start()
        joint(k, 1).start()

    def add_y(k):
        for g in (0, 1):
            joint(k, g).wait_recv()
            direct(k, g).wait_recv()
        for g in (0, 1):
            total = PG[k, 96:128, g * width : (g + 1) * width] + (SR[k, g].astype(F32) + SR[k, 2 + g].astype(F32))
            YB[k, 0, g] = total[0:16]
            YB[k, 1, g] = total[16:32]
        cross_sum(k).start()

    def activate(k):
        cross_sum(k).wait_recv()
        gate = YB[k, xl, 0] + XR[k, 0]
        up = YB[k, xl, 1] + XR[k, 1]
        HB[k, c, y, xl] = (gate / (1 + jnp.exp(-gate)) * up).astype(BF16)
        cross_h(k, xl).start()

    def spread_y(k):
        cross_h(k, 1 - xl).wait_recv()
        for send in spreads(k):
            send.start()

    def to_twin(k):
        for piece in spread_in(k):
            piece.wait_recv()
        twin_h(k, c).start()

    def down(k):
        twin_h(k, 1 - c).wait_recv()

        @pl.when(k == 0)
        def _():
            loads[3].wait()
            weight_in.wait_recv()

        @pl.loop(0, half // 256)
        def _(i):
            columns = pl.ds(pl.multiple_of(i * 256, 256), 256)
            own = jnp.dot(HB[k, 0].reshape(128, width), DW[0, :, columns], preferred_element_type=F32)
            total = own + jnp.dot(HB[k, 1].reshape(128, width), DW[1, :, columns], preferred_element_type=F32)
            PO[k, :, :, columns] = total.reshape(4, 32, 256)

        XS[k, 0] = PO[k, 1 - xh].astype(BF16)
        XS[k, 1] = PO[k, 3 - xh].astype(BF16)
        halves(k).start()

    def send_z(k):
        halves(k).wait_recv()
        totals = [PO[k, 2 * core + xh] + XD[k, core].astype(F32) for core in (0, 1)]

        @pl.when(k == 0)
        def _():
            FIN[0] = totals[0]
            FIN[1] = totals[1]

        @pl.when(k > 0)
        def _():
            ZS[k, 0] = totals[0].astype(BF16)
            ZS[k, 1] = totals[1].astype(BF16)
            home(k).start()

    stages = dict(gate_up=gate_up, relay_y=relay_y, add_y=add_y, activate=activate, spread_y=spread_y, to_twin=to_twin, down=down, send_z=send_z)

    def tick(i, carry):
        for name, lag in PLAN:

            @pl.when((i >= lag) & (i < lag + SLABS))
            def _():
                stages[name](i - lag)

        for n, when in enumerate(HOP_TICKS):

            @pl.when(i == when)
            def _():
                hop(n)

        return carry

    lax.fori_loop(0, SLABS + max(lag for _, lag in PLAN), tick, 0)

    for k in range(1, SLABS):
        home(k).wait_recv()
    out_copy = copy("out", 0, OS, OR, twin)
    for core in (0, 1):
        total = FIN[core]
        for k in range(1, SLABS):
            total += ZR[k, core].astype(F32)
        FIN[core] = total
    OS[...] = FIN[1 - c].astype(BF16)
    out_copy.start()
    out[:, pl.ds(mine, half)] = FIN[c].astype(BF16)
    out_copy.wait_recv()
    out[:, pl.ds(other, half)] = OR[...]

    pair_in(xh).wait_send()
    weight_out.wait_send()
    out_copy.wait_send()
    for n in range(4):
        ring_down(n).wait_send()
        ring_up(n).wait_send()

    def drain(k, carry):
        twin_in(k, c).wait_send()
        for g in (0, 1):
            far(k, g).wait_send()
            direct(k, g).wait_send()
            joint(k, g).wait_send()
        cross_sum(k).wait_send()
        cross_h(k, xl).wait_send()
        for send in spreads(k):
            send.wait_send()
        twin_h(k, c).wait_send()
        halves(k).wait_send()

        @pl.when(k > 0)
        def _():
            home(k).wait_send()

        return carry

    lax.fori_loop(0, SLABS, drain, 0)


def per_device(tokens, gate_weight, up_weight, down_weight):
    rows, depth = tokens.shape
    width = gate_weight.shape[1]
    half = down_weight.shape[1] // 2
    dma = pltpu.SemaphoreType.DMA
    return pl.pallas_call(
        kernel,
        out_shape=jax.ShapeDtypeStruct((rows, 2 * half), BF16),
        in_specs=[pl.BlockSpec(memory_space=pl.ANY)] * 4,
        out_specs=pl.BlockSpec(memory_space=pltpu.VMEM),
        scratch_shapes=[
            pltpu.VMEM((8, 4, rows, depth), BF16),
            pltpu.VMEM((depth, 2 * width), BF16),
            pltpu.VMEM((2, width, half), BF16),
            pltpu.VMEM((8, 128, 2 * width), F32),
            pltpu.VMEM((8, 2, 32, width), BF16),
            pltpu.VMEM((8, 2, 32, width), BF16),
            pltpu.VMEM((8, 4, 32, width), BF16),
            pltpu.VMEM((8, 4, 32, width), BF16),
            pltpu.VMEM((8, 2, 2, 16, width), F32),
            pltpu.VMEM((8, 2, 16, width), F32),
            pltpu.VMEM((8, 2, 4, 2, 16, width), BF16),
            pltpu.VMEM((8, 4, 32, half), F32),
            pltpu.VMEM((8, 2, 32, half), BF16),
            pltpu.VMEM((8, 2, 32, half), BF16),
            pltpu.VMEM((8, 2, 32, half), BF16),
            pltpu.VMEM((8, 2, 32, half), BF16),
            pltpu.VMEM((2, 32, half), F32),
            pltpu.VMEM((32, half), BF16),
            pltpu.VMEM((32, half), BF16),
            dma((4,)),
            dma((TOTAL,)),
            dma((TOTAL,)),
        ],
        compiler_params=pltpu.CompilerParams(collective_id=0, has_side_effects=True, vmem_limit_bytes=67043328),
        name="block",
    )(tokens, gate_weight, up_weight, down_weight)


def solution(mesh):
    return jax.shard_map(
        per_device,
        mesh=mesh,
        in_specs=(P("dp", "mp"), P("mp", "dp"), P("mp", "dp"), P("dp", "mp")),
        out_specs=P("dp", "mp"),
        check_vma=False,
    )
```

```python
import jax
import jax.numpy as jnp
from jax import lax
from jax.experimental import pallas as pl
from jax.experimental.pallas import tpu as pltpu
from jax.sharding import PartitionSpec as P


def arrive(copy):
    with jax.named_scope("wait"):
        copy.wait_recv()

MESH = pl.DeviceIdType.MESH
BF16, F32 = jnp.bfloat16, jnp.float32
SLABS = 8
PLACE = (0, 1, 2, 3, 4, 5, 6, 7)
STAGES = dict(g="gate_up", r="relay_y", a="add_y", s="activate", p="spread_y", t="to_twin", d="down", z="send_z")
ORDER = (
    "h00", "h01", "h10", "g0", "h11", "r0", "h20", "g1", "h21", "g7", "g6", "a0",
    "h30", "h31", "r1", "g2", "g3", "a1", "h40", "s0", "r6", "r2", "r3", "g4",
    "a6", "g5", "s1", "a3", "r4", "s6", "a2", "r5", "r7", "s3", "a4", "p6",
    "s2", "a5", "p3", "s4", "p0", "t6", "a7", "p4", "p1", "t3", "s5", "d6",
    "d3", "t0", "p5", "p2", "t4", "s7", "z6", "d4", "t5", "z3", "p7", "t2",
    "d5", "z4", "t1", "d2", "t7", "d1", "z5", "d7", "d0", "z2", "z1", "z7",
    "z0",
)
FIRST_DOWN = next(step for step in ORDER if step[0] == "d")

COPIES = dict(
    pair=1, up_ring=8, down_ring=8, twin_in=16,
    far=16, direct=16, joint=16, cross=8, cross_h=8, spread=24, twin_h=8,
    half=8, home=8, out=1, weight=1,
)
BASE, TOTAL = {}, 0
for _name, _count in COPIES.items():
    BASE[_name], TOTAL = TOTAL, TOTAL + _count


def kernel(tokens, gate_w, up_w, down_w, out, T, GU, DW, PG, FS, FR, SS, SR, YB, XR, HB, PO, XS, XD, ZS, ZR, FIN, OS, OR, local, sent, got):
    dp, mp = lax.axis_index("dp"), lax.axis_index("mp")
    z, xh, c = dp // 4, (dp // 2) & 1, dp & 1
    xl, y = mp // 4, mp & 3
    width = gate_w.shape[1]
    half = DW.shape[2]

    def device(z_=z, xh_=xh, c_=c, xl_=xl, y_=y):
        return (z_ * 4 + xh_ * 2 + c_, xl_ * 4 + y_)

    twin = device(c_=1 - c)
    pair = device(xh_=1 - xh)
    cross = device(xl_=1 - xl)
    y_up, y_down, y_far = (device(y_=(y + n) & 3) for n in (1, 3, 2))

    def at_z(n):
        return device(z_=(z + n) & 7)

    mine = pl.multiple_of(c * half, half)
    other = pl.multiple_of((1 - c) * half, half)
    loads = [
        pltpu.make_async_copy(tokens, T.at[z, 2 * c + xh], local.at[0]),
        pltpu.make_async_copy(gate_w, GU.at[:, pl.ds(0, width)], local.at[1]),
        pltpu.make_async_copy(up_w, GU.at[:, pl.ds(width, width)], local.at[2]),
        pltpu.make_async_copy(down_w.at[:, pl.ds(mine, half)], DW.at[c], local.at[3]),
    ]
    for load in loads:
        load.start()

    barrier = pltpu.get_barrier_semaphore()
    friends = [twin, pair, cross, y_up, y_down, y_far] + [at_z(n) for n in range(1, 8)]
    for friend in friends:
        pl.semaphore_signal(barrier, inc=1, device_id=friend, device_id_type=MESH)
    pl.semaphore_wait(barrier, len(friends))

    def copy(name, n, src, dst, to, lands=None):
        return pltpu.make_async_remote_copy(
            src_ref=src,
            dst_ref=dst,
            send_sem=sent.at[BASE[name] + n],
            recv_sem=got.at[BASE[name] + (n if lands is None else lands)],
            device_id=to,
            device_id_type=MESH,
        )

    def slab(n):
        return (z + n) & 7

    def piece(n, part, core):
        return T.at[slab(n), 2 * core + (1 - xh if part else xh)]

    def ring_down(hop, part):
        ref = piece(hop, part, c)
        return copy("down_ring", 2 * hop + part, ref, ref, at_z(7))

    def ring_up(hop, part):
        ref = piece(-hop, part, c)
        return copy("up_ring", 2 * hop + part, ref, ref, at_z(1))

    def from_above(hop, part):
        ref = piece(hop + 1, part, c)
        return copy("down_ring", 2 * hop + part, ref, ref, at_z(1))

    def from_below(hop, part):
        ref = piece(-hop - 1, part, c)
        return copy("up_ring", 2 * hop + part, ref, ref, at_z(7))

    def twin_in(n, part, core):
        row = 1 - xh if part else xh
        ref = T.at[slab(n), 2 * core + row]
        return copy("twin_in", 2 * (n % 8) + part, ref, ref, twin)

    def pair_in(part):
        ref = piece(0, part, c)
        return copy("pair", 0, ref, ref, pair)

    weight_out = copy("weight", 0, down_w.at[:, pl.ds(other, half)], DW.at[c], twin)
    weight_in = copy("weight", 0, DW.at[1 - c], DW.at[1 - c], twin)

    def hop(n, part):
        if n == 0:
            if part == 0:
                loads[0].wait()
                pair_in(0).start()
            else:
                arrive(pair_in(1))
            ring_down(0, part).start()
            ring_up(0, part).start()
            twin_in(0, part, c).start()
            if part == 1:
                weight_out.start()
        elif n < 4:
            arrive(from_above(n - 1, part))
            arrive(from_below(n - 1, part))
            if n < 3 or part == 0:
                ring_down(n, part).start()
            if n < 3 or part == 1:
                ring_up(n, part).start()
            twin_in(n, part, c).start()
            twin_in(-n, part, c).start()
        else:
            arrive(from_above(3, 0))
            arrive(from_below(3, 1))
            twin_in(4, 0, c).start()
            twin_in(4, 1, c).start()

    def far(k, g):
        return copy("far", 2 * k + g, FS.at[k, g], FR.at[k, g], y_down if g else y_up)

    def joint(k, g):
        return copy("joint", 2 * k + g, SS.at[k, g], SR.at[k, g], y_down if g else y_up)

    def direct(k, g):
        return copy("direct", 2 * k + g, SS.at[k, 2 + g], SR.at[k, 2 + g], y_up if g else y_down)

    def cross_sum(k):
        return copy("cross", k, YB.at[k, 1 - xl], XR.at[k], cross)

    def cross_h(k, x):
        ref = HB.at[k, c, y, x]
        return copy("cross_h", k, ref, ref, cross)

    def spread(k, n, row, to):
        ref = HB.at[k, c, row]
        return copy("spread", 3 * k + n, ref, ref, to)

    def spreads(k):
        return [spread(k, n, y, to) for n, to in enumerate((y_up, y_down, y_far))]

    def spread_in(k):
        return [spread(k, n, (y + m) & 3, y_far) for n, m in enumerate((3, 1, 2))]

    def twin_h(k, core):
        ref = HB.at[k, core]
        return copy("twin_h", k, ref, ref, twin)

    def halves(k):
        return copy("half", k, XS.at[k], XD.at[k], pair)

    def home(k):
        return copy("home", k, ZS.at[k], ZR.at[k], at_z(PLACE[k]))

    def gate_up(k):
        n = PLACE[k]
        s = slab(n)
        arrive(twin_in(n, 0, 1 - c))
        arrive(twin_in(n, 1, 1 - c))
        if k == 0:
            loads[1].wait()
            loads[2].wait()

        @pl.loop(0, 7)
        def _(i):
            columns = pl.ds(pl.multiple_of(i * 256, 256), 256)
            rows = jnp.concatenate([T[s, (y + m) & 3] for m in (2, 1, 3, 0)], axis=0)
            PG[k, :, columns] = jnp.dot(rows, GU[:, columns], preferred_element_type=F32)

        FS[k, 0] = PG[k, 0:32, 0:width].astype(BF16)
        FS[k, 1] = PG[k, 0:32, width:].astype(BF16)
        far(k, 0).start()
        far(k, 1).start()
        SS[k, 2] = PG[k, 64:96, 0:width].astype(BF16)
        SS[k, 3] = PG[k, 32:64, width:].astype(BF16)
        direct(k, 0).start()
        direct(k, 1).start()

    def relay_y(k):
        arrive(far(k, 0))
        arrive(far(k, 1))
        SS[k, 0] = (PG[k, 32:64, 0:width] + FR[k, 0].astype(F32)).astype(BF16)
        SS[k, 1] = (PG[k, 64:96, width:] + FR[k, 1].astype(F32)).astype(BF16)
        joint(k, 0).start()
        joint(k, 1).start()

    def add_y(k):
        for g in (0, 1):
            arrive(joint(k, g))
            arrive(direct(k, g))
        for g in (0, 1):
            total = PG[k, 96:128, g * width : (g + 1) * width] + (SR[k, g].astype(F32) + SR[k, 2 + g].astype(F32))
            YB[k, 0, g] = total[0:16]
            YB[k, 1, g] = total[16:32]
        cross_sum(k).start()

    def activate(k):
        arrive(cross_sum(k))
        gate = YB[k, xl, 0] + XR[k, 0]
        up = YB[k, xl, 1] + XR[k, 1]
        HB[k, c, y, xl] = (gate / (1 + jnp.exp(-gate)) * up).astype(BF16)
        cross_h(k, xl).start()

    def spread_y(k):
        arrive(cross_h(k, 1 - xl))
        for send in spreads(k):
            send.start()

    def to_twin(k):
        for piece in spread_in(k):
            arrive(piece)
        twin_h(k, c).start()

    def down(k):
        arrive(twin_h(k, 1 - c))

        if "d%d" % k == FIRST_DOWN:
            loads[3].wait()
            arrive(weight_in)

        @pl.loop(0, half // 256)
        def _(i):
            columns = pl.ds(pl.multiple_of(i * 256, 256), 256)
            own = jnp.dot(HB[k, 0].reshape(128, width), DW[0, :, columns], preferred_element_type=F32)
            total = own + jnp.dot(HB[k, 1].reshape(128, width), DW[1, :, columns], preferred_element_type=F32)
            PO[k, :, :, columns] = total.reshape(4, 32, 256)

        XS[k, 0] = PO[k, 1 - xh].astype(BF16)
        XS[k, 1] = PO[k, 3 - xh].astype(BF16)
        halves(k).start()

    def send_z(k):
        arrive(halves(k))
        totals = [PO[k, 2 * core + xh] + XD[k, core].astype(F32) for core in (0, 1)]

        if k == 0:
            FIN[0] = totals[0]
            FIN[1] = totals[1]
        else:
            ZS[k, 0] = totals[0].astype(BF16)
            ZS[k, 1] = totals[1].astype(BF16)
            home(k).start()

    stages = dict(gate_up=gate_up, relay_y=relay_y, add_y=add_y, activate=activate, spread_y=spread_y, to_twin=to_twin, down=down, send_z=send_z)

    for step in ORDER:
        if step[0] == "h":
            with jax.named_scope(step):
                hop(int(step[1]), int(step[2]))
        else:
            with jax.named_scope(step + STAGES[step[0]]):
                stages[STAGES[step[0]]](int(step[1]))

    for k in range(1, SLABS):
        arrive(home(k))
    out_copy = copy("out", 0, OS, OR, twin)
    for core in (0, 1):
        total = FIN[core]
        for k in range(1, SLABS):
            total += ZR[k, core].astype(F32)
        FIN[core] = total
    OS[...] = FIN[1 - c].astype(BF16)
    out_copy.start()
    out[:, pl.ds(mine, half)] = FIN[c].astype(BF16)
    arrive(out_copy)
    out[:, pl.ds(other, half)] = OR[...]

    pair_in(0).wait_send()
    weight_out.wait_send()
    out_copy.wait_send()
    for part in (0, 1):
        for n in range(3):
            ring_down(n, part).wait_send()
            ring_up(n, part).wait_send()
    ring_down(3, 0).wait_send()
    ring_up(3, 1).wait_send()
    for k in range(SLABS):
        for g in (0, 1):
            twin_in(k, g, c).wait_send()
            far(k, g).wait_send()
            direct(k, g).wait_send()
            joint(k, g).wait_send()
        cross_sum(k).wait_send()
        cross_h(k, xl).wait_send()
        for send in spreads(k):
            send.wait_send()
        twin_h(k, c).wait_send()
        halves(k).wait_send()
        if k > 0:
            home(k).wait_send()


def per_device(tokens, gate_weight, up_weight, down_weight):
    rows, depth = tokens.shape
    width = gate_weight.shape[1]
    half = down_weight.shape[1] // 2
    dma = pltpu.SemaphoreType.DMA
    return pl.pallas_call(
        kernel,
        out_shape=jax.ShapeDtypeStruct((rows, 2 * half), BF16),
        in_specs=[pl.BlockSpec(memory_space=pl.ANY)] * 4,
        out_specs=pl.BlockSpec(memory_space=pltpu.VMEM),
        scratch_shapes=[
            pltpu.VMEM((8, 4, rows, depth), BF16),
            pltpu.VMEM((depth, 2 * width), BF16),
            pltpu.VMEM((2, width, half), BF16),
            pltpu.VMEM((8, 128, 2 * width), F32),
            pltpu.VMEM((8, 2, 32, width), BF16),
            pltpu.VMEM((8, 2, 32, width), BF16),
            pltpu.VMEM((8, 4, 32, width), BF16),
            pltpu.VMEM((8, 4, 32, width), BF16),
            pltpu.VMEM((8, 2, 2, 16, width), F32),
            pltpu.VMEM((8, 2, 16, width), F32),
            pltpu.VMEM((8, 2, 4, 2, 16, width), BF16),
            pltpu.VMEM((8, 4, 32, half), F32),
            pltpu.VMEM((8, 2, 32, half), BF16),
            pltpu.VMEM((8, 2, 32, half), BF16),
            pltpu.VMEM((8, 2, 32, half), BF16),
            pltpu.VMEM((8, 2, 32, half), BF16),
            pltpu.VMEM((2, 32, half), F32),
            pltpu.VMEM((32, half), BF16),
            pltpu.VMEM((32, half), BF16),
            dma((4,)),
            dma((TOTAL,)),
            dma((TOTAL,)),
        ],
        compiler_params=pltpu.CompilerParams(collective_id=0, has_side_effects=True, vmem_limit_bytes=67043328),
        name="block",
    )(tokens, gate_weight, up_weight, down_weight)


def solution(mesh):
    return jax.shard_map(
        per_device,
        mesh=mesh,
        in_specs=(P("dp", "mp"), P("mp", "dp"), P("mp", "dp"), P("dp", "mp")),
        out_specs=P("dp", "mp"),
        check_vma=False,
    )
```

```python
import jax
import jax.numpy as jnp
from jax import lax
from jax.experimental import pallas as pl
from jax.experimental.pallas import tpu as pltpu
from jax.sharding import PartitionSpec as P


def arrive(copy):
    with jax.named_scope("wait"):
        copy.wait_recv()

MESH = pl.DeviceIdType.MESH
BF16, F32 = jnp.bfloat16, jnp.float32
SLABS = 8
PLACE = (0, 1, 7, 2, 6, 3, 5, 4)
STAGES = dict(g="gate_up", r="relay_y", a="add_y", s="activate", p="spread_y", t="to_twin", d="down", z="send_z", y="send_other_z")
ORDER = (
    "h00", "h01", "h10", "g0", "h11", "r0", "h20", "g1", "h21", "g2", "a0", "g4",
    "h31", "h30", "r1", "r2", "r4", "g5", "a1", "h40", "g6", "a4", "a2", "r5",
    "g7", "r6", "g3", "s4", "a5", "r7", "s0", "a6", "p4", "s5", "r3", "a7",
    "s6", "s2", "p5", "t4", "a3", "s7", "p6", "d4", "t5", "s3", "p7", "s1",
    "p2", "d5", "t6", "z4", "y4", "p3", "d6", "p1", "t7", "z5", "t2", "d7",
    "y5", "p0", "t3", "z6", "d3", "y6", "t1", "z7", "d2", "y7", "t0", "d1",
    "z3", "d0", "y2", "y3", "z2", "y1", "z0", "z1", "y0",
)
FIRST_DOWN = next(step for step in ORDER if step[0] == "d")

COPIES = dict(
    pair=1, up_ring=8, down_ring=8, twin_in=16,
    far=16, direct=16, joint=16, cross=8, cross_h=8, spread=24, twin_h=8,
    half=16, home=16, own=1, weight=1,
)
BASE, TOTAL = {}, 0
for _name, _count in COPIES.items():
    BASE[_name], TOTAL = TOTAL, TOTAL + _count


def kernel(tokens, gate_w, up_w, down_w, out, T, GU, DW, PG, FS, FR, SS, SR, YB, XR, HB, PO, XS, XD, ZS, ZR, FIN, OTHER, local, sent, got):
    dp, mp = lax.axis_index("dp"), lax.axis_index("mp")
    z, xh, c = dp // 4, (dp // 2) & 1, dp & 1
    xl, y = mp // 4, mp & 3
    width = gate_w.shape[1]
    half = DW.shape[2]

    def device(z_=z, xh_=xh, c_=c, xl_=xl, y_=y):
        return (z_ * 4 + xh_ * 2 + c_, xl_ * 4 + y_)

    twin = device(c_=1 - c)
    pair = device(xh_=1 - xh)
    cross = device(xl_=1 - xl)
    y_up, y_down, y_far = (device(y_=(y + n) & 3) for n in (1, 3, 2))

    def at_z(n, core=c):
        return device(z_=(z + n) & 7, c_=core)

    mine = pl.multiple_of(c * half, half)
    other = pl.multiple_of((1 - c) * half, half)
    loads = [
        pltpu.make_async_copy(tokens, T.at[z, 2 * c + xh], local.at[0]),
        pltpu.make_async_copy(gate_w, GU.at[:, pl.ds(0, width)], local.at[1]),
        pltpu.make_async_copy(up_w, GU.at[:, pl.ds(width, width)], local.at[2]),
        pltpu.make_async_copy(down_w.at[:, pl.ds(mine, half)], DW.at[c], local.at[3]),
    ]
    for load in loads:
        load.start()

    barrier = pltpu.get_barrier_semaphore()
    friends = [twin, pair, cross, y_up, y_down, y_far] + [at_z(n, core) for n in range(1, 8) for core in (c, 1 - c)]
    for friend in friends:
        pl.semaphore_signal(barrier, inc=1, device_id=friend, device_id_type=MESH)
    pl.semaphore_wait(barrier, len(friends))

    def copy(name, n, src, dst, to, lands=None):
        return pltpu.make_async_remote_copy(
            src_ref=src,
            dst_ref=dst,
            send_sem=sent.at[BASE[name] + n],
            recv_sem=got.at[BASE[name] + (n if lands is None else lands)],
            device_id=to,
            device_id_type=MESH,
        )

    def slab(n):
        return (z + n) & 7

    def piece(n, part, core):
        return T.at[slab(n), 2 * core + (1 - xh if part else xh)]

    def ring_down(hop, part):
        ref = piece(hop, part, c)
        return copy("down_ring", 2 * hop + part, ref, ref, at_z(7))

    def ring_up(hop, part):
        ref = piece(-hop, part, c)
        return copy("up_ring", 2 * hop + part, ref, ref, at_z(1))

    def from_above(hop, part):
        ref = piece(hop + 1, part, c)
        return copy("down_ring", 2 * hop + part, ref, ref, at_z(1))

    def from_below(hop, part):
        ref = piece(-hop - 1, part, c)
        return copy("up_ring", 2 * hop + part, ref, ref, at_z(7))

    def twin_in(n, part, core):
        row = 1 - xh if part else xh
        ref = T.at[slab(n), 2 * core + row]
        return copy("twin_in", 2 * (n % 8) + part, ref, ref, twin)

    def pair_in(part):
        ref = piece(0, part, c)
        return copy("pair", 0, ref, ref, pair)

    weight_out = copy("weight", 0, down_w.at[:, pl.ds(other, half)], DW.at[c], twin)
    weight_in = copy("weight", 0, DW.at[1 - c], DW.at[1 - c], twin)

    def hop(n, part):
        if n == 0:
            if part == 0:
                loads[0].wait()
                pair_in(0).start()
            else:
                arrive(pair_in(1))
            ring_down(0, part).start()
            ring_up(0, part).start()
            twin_in(0, part, c).start()
            if part == 1:
                weight_out.start()
        elif n < 4:
            arrive(from_above(n - 1, part))
            arrive(from_below(n - 1, part))
            if n < 3 or part == 0:
                ring_down(n, part).start()
            if n < 3 or part == 1:
                ring_up(n, part).start()
            twin_in(n, part, c).start()
            twin_in(-n, part, c).start()
        else:
            arrive(from_above(3, 0))
            arrive(from_below(3, 1))
            twin_in(4, 0, c).start()
            twin_in(4, 1, c).start()

    def far(k, g):
        return copy("far", 2 * k + g, FS.at[k, g], FR.at[k, g], y_down if g else y_up)

    def joint(k, g):
        return copy("joint", 2 * k + g, SS.at[k, g], SR.at[k, g], y_down if g else y_up)

    def direct(k, g):
        return copy("direct", 2 * k + g, SS.at[k, 2 + g], SR.at[k, 2 + g], y_up if g else y_down)

    def cross_sum(k):
        return copy("cross", k, YB.at[k, 1 - xl], XR.at[k], cross)

    def cross_h(k, x):
        ref = HB.at[k, c, y, x]
        return copy("cross_h", k, ref, ref, cross)

    def spread(k, n, row, to):
        ref = HB.at[k, c, row]
        return copy("spread", 3 * k + n, ref, ref, to)

    def spreads(k):
        return [spread(k, n, y, to) for n, to in enumerate((y_up, y_down, y_far))]

    def spread_in(k):
        return [spread(k, n, (y + m) & 3, y_far) for n, m in enumerate((3, 1, 2))]

    def twin_h(k, core):
        ref = HB.at[k, core]
        return copy("twin_h", k, ref, ref, twin)

    def core_of(part):
        return 1 - c if part else c

    def halves(k, part):
        return copy("half", 2 * k + part, XS.at[k, part], XD.at[k, part], pair)

    def home(k, part):
        return copy("home", 2 * k + part, ZS.at[k, part], ZR.at[k, part], at_z(PLACE[k], core_of(part)))

    own_copy = copy("own", 0, FIN.at[1], OTHER, twin)

    def gate_up(k):
        n = PLACE[k]
        s = slab(n)
        arrive(twin_in(n, 0, 1 - c))
        arrive(twin_in(n, 1, 1 - c))
        if k == 0:
            loads[1].wait()
            loads[2].wait()

        @pl.loop(0, 7)
        def _(i):
            columns = pl.ds(pl.multiple_of(i * 256, 256), 256)
            rows = jnp.concatenate([T[s, (y + m) & 3] for m in (2, 1, 3, 0)], axis=0)
            PG[k, :, columns] = jnp.dot(rows, GU[:, columns], preferred_element_type=F32)

        FS[k, 0] = PG[k, 0:32, 0:width].astype(BF16)
        FS[k, 1] = PG[k, 0:32, width:].astype(BF16)
        far(k, 0).start()
        far(k, 1).start()
        SS[k, 2] = PG[k, 64:96, 0:width].astype(BF16)
        SS[k, 3] = PG[k, 32:64, width:].astype(BF16)
        direct(k, 0).start()
        direct(k, 1).start()

    def relay_y(k):
        arrive(far(k, 0))
        arrive(far(k, 1))
        SS[k, 0] = (PG[k, 32:64, 0:width] + FR[k, 0].astype(F32)).astype(BF16)
        SS[k, 1] = (PG[k, 64:96, width:] + FR[k, 1].astype(F32)).astype(BF16)
        joint(k, 0).start()
        joint(k, 1).start()

    def add_y(k):
        for g in (0, 1):
            arrive(joint(k, g))
            arrive(direct(k, g))
        for g in (0, 1):
            total = PG[k, 96:128, g * width : (g + 1) * width] + (SR[k, g].astype(F32) + SR[k, 2 + g].astype(F32))
            YB[k, 0, g] = total[0:16]
            YB[k, 1, g] = total[16:32]
        cross_sum(k).start()

    def activate(k):
        arrive(cross_sum(k))
        gate = YB[k, xl, 0] + XR[k, 0]
        up = YB[k, xl, 1] + XR[k, 1]
        HB[k, c, y, xl] = (gate / (1 + jnp.exp(-gate)) * up).astype(BF16)
        cross_h(k, xl).start()

    def spread_y(k):
        arrive(cross_h(k, 1 - xl))
        for send in spreads(k):
            send.start()

    def to_twin(k):
        for piece in spread_in(k):
            arrive(piece)
        twin_h(k, c).start()

    def down(k):
        arrive(twin_h(k, 1 - c))

        if "d%d" % k == FIRST_DOWN:
            loads[3].wait()
            arrive(weight_in)

        @pl.loop(0, half // 256)
        def _(i):
            columns = pl.ds(pl.multiple_of(i * 256, 256), 256)
            own = jnp.dot(HB[k, 0].reshape(128, width), DW[0, :, columns], preferred_element_type=F32)
            total = own + jnp.dot(HB[k, 1].reshape(128, width), DW[1, :, columns], preferred_element_type=F32)
            PO[k, :, :, columns] = total.reshape(4, 32, 256)

        for part in (0, 1):
            XS[k, part] = PO[k, 2 * core_of(part) + 1 - xh].astype(BF16)
            halves(k, part).start()

    def send_part(k, part):
        arrive(halves(k, part))
        total = PO[k, 2 * core_of(part) + xh] + XD[k, part].astype(F32)
        if k == 0:
            FIN[part] = total
            if part == 1:
                own_copy.start()
        else:
            ZS[k, part] = total.astype(BF16)
            home(k, part).start()

    def send_z(k):
        send_part(k, 0)

    def send_other_z(k):
        send_part(k, 1)

    stages = dict(gate_up=gate_up, relay_y=relay_y, add_y=add_y, activate=activate, spread_y=spread_y, to_twin=to_twin, down=down, send_z=send_z, send_other_z=send_other_z)

    for step in ORDER:
        if step[0] == "h":
            with jax.named_scope(step):
                hop(int(step[1]), int(step[2]))
        else:
            with jax.named_scope(step + STAGES[step[0]]):
                stages[STAGES[step[0]]](int(step[1]))

    pair_in(0).wait_send()
    weight_out.wait_send()
    own_copy.wait_send()
    for part in (0, 1):
        for n in range(3):
            ring_down(n, part).wait_send()
            ring_up(n, part).wait_send()
    ring_down(3, 0).wait_send()
    ring_up(3, 1).wait_send()
    for k in range(SLABS):
        for g in (0, 1):
            twin_in(k, g, c).wait_send()
            far(k, g).wait_send()
            direct(k, g).wait_send()
            joint(k, g).wait_send()
        cross_sum(k).wait_send()
        cross_h(k, xl).wait_send()
        for send in spreads(k):
            send.wait_send()
        twin_h(k, c).wait_send()
        for part in (0, 1):
            halves(k, part).wait_send()

    arrive(own_copy)
    for k in range(1, SLABS):
        arrive(home(k, 0))
        arrive(home(k, 1))
    for part, (first, columns) in enumerate(((FIN.at[0], mine), (OTHER, other))):
        total = first[...]
        for k in range(1, SLABS):
            total += ZR[k, part].astype(F32)
        out[:, pl.ds(columns, half)] = total.astype(BF16)
    for k in range(1, SLABS):
        home(k, 0).wait_send()
        home(k, 1).wait_send()


def per_device(tokens, gate_weight, up_weight, down_weight):
    rows, depth = tokens.shape
    width = gate_weight.shape[1]
    half = down_weight.shape[1] // 2
    dma = pltpu.SemaphoreType.DMA
    return pl.pallas_call(
        kernel,
        out_shape=jax.ShapeDtypeStruct((rows, 2 * half), BF16),
        in_specs=[pl.BlockSpec(memory_space=pl.ANY)] * 4,
        out_specs=pl.BlockSpec(memory_space=pltpu.VMEM),
        scratch_shapes=[
            pltpu.VMEM((8, 4, rows, depth), BF16),
            pltpu.VMEM((depth, 2 * width), BF16),
            pltpu.VMEM((2, width, half), BF16),
            pltpu.VMEM((8, 128, 2 * width), F32),
            pltpu.VMEM((8, 2, 32, width), BF16),
            pltpu.VMEM((8, 2, 32, width), BF16),
            pltpu.VMEM((8, 4, 32, width), BF16),
            pltpu.VMEM((8, 4, 32, width), BF16),
            pltpu.VMEM((8, 2, 2, 16, width), F32),
            pltpu.VMEM((8, 2, 16, width), F32),
            pltpu.VMEM((8, 2, 4, 2, 16, width), BF16),
            pltpu.VMEM((8, 4, 32, half), F32),
            pltpu.VMEM((8, 2, 32, half), BF16),
            pltpu.VMEM((8, 2, 32, half), BF16),
            pltpu.VMEM((8, 2, 32, half), BF16),
            pltpu.VMEM((8, 2, 32, half), BF16),
            pltpu.VMEM((2, 32, half), F32),
            pltpu.VMEM((32, half), F32),
            dma((4,)),
            dma((TOTAL,)),
            dma((TOTAL,)),
        ],
        compiler_params=pltpu.CompilerParams(collective_id=0, has_side_effects=True, vmem_limit_bytes=67043328),
        name="block",
    )(tokens, gate_weight, up_weight, down_weight)


def solution(mesh):
    return jax.shard_map(
        per_device,
        mesh=mesh,
        in_specs=(P("dp", "mp"), P("mp", "dp"), P("mp", "dp"), P("dp", "mp")),
        out_specs=P("dp", "mp"),
        check_vma=False,
    )
```

```python
import jax
import jax.numpy as jnp
from jax import lax
from jax.experimental import pallas as pl
from jax.experimental.pallas import tpu as pltpu
from jax.sharding import PartitionSpec as P


def arrive(copy):
    with jax.named_scope("wait"):
        copy.wait_recv()

MESH = pl.DeviceIdType.MESH
BF16, F32 = jnp.bfloat16, jnp.float32
SLABS = 8
PLACE = (0, 1, 7, 2, 6, 3, 5, 4)
STAGES = dict(g="gate_up", r="relay_y", a="add_y", s="activate", p="spread_y", t="to_twin", d="down", z="send_z", y="send_other_z")
ORDER = (
    "h00", "h01", "h10", "g0", "h11", "r0", "h20", "g1", "h21", "g2", "a0", "g4",
    "h31", "h30", "r1", "r2", "r4", "g5", "a1", "h40", "g6", "a4", "a2", "r5",
    "g7", "r6", "g3", "s4", "a5", "r7", "s0", "a6", "p4", "s5", "r3", "a7",
    "s6", "s2", "p5", "t4", "a3", "s7", "p6", "d4", "t5", "s3", "p7", "s1",
    "p2", "d5", "t6", "z4", "y4", "p3", "d6", "p1", "t7", "z5", "t2", "d7",
    "y5", "p0", "t3", "z6", "d3", "y6", "t1", "z7", "d2", "y7", "t0", "d1",
    "z3", "d0", "y2", "y3", "z2", "y1", "z0", "z1", "y0",
)
FIRST_DOWN = next(step for step in ORDER if step[0] == "d")

COPIES = dict(
    pair=1, up_ring=8, down_ring=8, twin_in=16,
    far=16, direct=16, joint=16, cross=8, cross_h=8, spread=24, twin_h=8,
    half=16, home=16, own=1, weight=1,
)
BASE, TOTAL = {}, 0
for _name, _count in COPIES.items():
    BASE[_name], TOTAL = TOTAL, TOTAL + _count


def kernel(tokens, gate_w, up_w, down_w, out, T, GU, DW, PG, FS, FR, SS, SR, YB, XR, HB, PO, XS, XD, ZS, ZR, FIN, OTHER, local, sent, got):
    dp, mp = lax.axis_index("dp"), lax.axis_index("mp")
    z, xh, c = dp // 4, (dp // 2) & 1, dp & 1
    xl, y = mp // 4, mp & 3
    width = gate_w.shape[1]
    half = DW.shape[2]

    def device(z_=z, xh_=xh, c_=c, xl_=xl, y_=y):
        return (z_ * 4 + xh_ * 2 + c_, xl_ * 4 + y_)

    twin = device(c_=1 - c)
    pair = device(xh_=1 - xh)
    cross = device(xl_=1 - xl)
    y_up, y_down, y_far = (device(y_=(y + n) & 3) for n in (1, 3, 2))

    def at_z(n, core=c):
        return device(z_=(z + n) & 7, c_=core)

    mine = pl.multiple_of(c * half, half)
    other = pl.multiple_of((1 - c) * half, half)
    loads = [
        pltpu.make_async_copy(tokens, T.at[z, 2 * c + xh], local.at[0]),
        pltpu.make_async_copy(gate_w, GU.at[:, pl.ds(0, width)], local.at[1]),
        pltpu.make_async_copy(up_w, GU.at[:, pl.ds(width, width)], local.at[2]),
        pltpu.make_async_copy(down_w.at[:, pl.ds(mine, half)], DW.at[c], local.at[3]),
    ]
    for load in loads:
        load.start()

    barrier = pltpu.get_barrier_semaphore()
    friends = [twin, pair, cross, y_up, y_down, y_far] + [at_z(n, core) for n in range(1, 8) for core in (c, 1 - c)]
    for friend in friends:
        pl.semaphore_signal(barrier, inc=1, device_id=friend, device_id_type=MESH)
    pl.semaphore_wait(barrier, len(friends))

    def copy(name, n, src, dst, to, lands=None):
        return pltpu.make_async_remote_copy(
            src_ref=src,
            dst_ref=dst,
            send_sem=sent.at[BASE[name] + n],
            recv_sem=got.at[BASE[name] + (n if lands is None else lands)],
            device_id=to,
            device_id_type=MESH,
        )

    def slab(n):
        return (z + n) & 7

    def piece(n, part, core):
        return T.at[slab(n), 2 * core + (1 - xh if part else xh)]

    def ring_down(hop, part):
        ref = piece(hop, part, c)
        return copy("down_ring", 2 * hop + part, ref, ref, at_z(7))

    def ring_up(hop, part):
        ref = piece(-hop, part, c)
        return copy("up_ring", 2 * hop + part, ref, ref, at_z(1))

    def from_above(hop, part):
        ref = piece(hop + 1, part, c)
        return copy("down_ring", 2 * hop + part, ref, ref, at_z(1))

    def from_below(hop, part):
        ref = piece(-hop - 1, part, c)
        return copy("up_ring", 2 * hop + part, ref, ref, at_z(7))

    def twin_in(n, part, core):
        row = 1 - xh if part else xh
        ref = T.at[slab(n), 2 * core + row]
        return copy("twin_in", 2 * (n % 8) + part, ref, ref, twin)

    def pair_in(part):
        ref = piece(0, part, c)
        return copy("pair", 0, ref, ref, pair)

    weight_out = copy("weight", 0, down_w.at[:, pl.ds(other, half)], DW.at[c], twin)
    weight_in = copy("weight", 0, DW.at[1 - c], DW.at[1 - c], twin)

    def hop(n, part):
        if n == 0:
            if part == 0:
                loads[0].wait()
                pair_in(0).start()
            else:
                arrive(pair_in(1))
            ring_down(0, part).start()
            ring_up(0, part).start()
            twin_in(0, part, c).start()
            if part == 1:
                weight_out.start()
        elif n < 4:
            arrive(from_above(n - 1, part))
            arrive(from_below(n - 1, part))
            if n < 3 or part == 0:
                ring_down(n, part).start()
            if n < 3 or part == 1:
                ring_up(n, part).start()
            twin_in(n, part, c).start()
            twin_in(-n, part, c).start()
        else:
            arrive(from_above(3, 0))
            arrive(from_below(3, 1))
            twin_in(4, 0, c).start()
            twin_in(4, 1, c).start()

    def far(k, g):
        return copy("far", 2 * k + g, FS.at[k, g], FR.at[k, g], y_down if g else y_up)

    def joint(k, g):
        return copy("joint", 2 * k + g, SS.at[k, g], SR.at[k, g], y_down if g else y_up)

    def direct(k, g):
        return copy("direct", 2 * k + g, SS.at[k, 2 + g], SR.at[k, 2 + g], y_up if g else y_down)

    def cross_sum(k):
        return copy("cross", k, YB.at[k, 1 - xl], XR.at[k], cross)

    def cross_h(k, x):
        ref = HB.at[k, c, y, x]
        return copy("cross_h", k, ref, ref, cross)

    def spread(k, n, row, to):
        ref = HB.at[k, c, row]
        return copy("spread", 3 * k + n, ref, ref, to)

    def spreads(k):
        return [spread(k, n, y, to) for n, to in enumerate((y_up, y_down, y_far))]

    def spread_in(k):
        return [spread(k, n, (y + m) & 3, y_far) for n, m in enumerate((3, 1, 2))]

    def twin_h(k, core):
        ref = HB.at[k, core]
        return copy("twin_h", k, ref, ref, twin)

    def core_of(part):
        return 1 - c if part else c

    def halves(k, part):
        return copy("half", 2 * k + part, XS.at[k, part], XD.at[k, part], pair)

    def home(k, part):
        return copy("home", 2 * k + part, ZS.at[k, part], ZR.at[k, part], at_z(PLACE[k], core_of(part)))

    own_copy = copy("own", 0, FIN.at[1], OTHER, twin)

    def gate_up(k):
        n = PLACE[k]
        s = slab(n)
        arrive(twin_in(n, 0, 1 - c))
        arrive(twin_in(n, 1, 1 - c))
        if k == 0:
            loads[1].wait()
            loads[2].wait()

        @pl.loop(0, 7, unroll=True)
        def _(i):
            columns = pl.ds(pl.multiple_of(i * 256, 256), 256)
            rows = jnp.concatenate([T[s, (y + m) & 3] for m in (2, 1, 3, 0)], axis=0)
            PG[k, :, columns] = jnp.dot(rows, GU[:, columns], preferred_element_type=F32)

        FS[k, 0] = PG[k, 0:32, 0:width].astype(BF16)
        FS[k, 1] = PG[k, 0:32, width:].astype(BF16)
        far(k, 0).start()
        far(k, 1).start()
        SS[k, 2] = PG[k, 64:96, 0:width].astype(BF16)
        SS[k, 3] = PG[k, 32:64, width:].astype(BF16)
        direct(k, 0).start()
        direct(k, 1).start()

    def relay_y(k):
        arrive(far(k, 0))
        arrive(far(k, 1))
        SS[k, 0] = (PG[k, 32:64, 0:width] + FR[k, 0].astype(F32)).astype(BF16)
        SS[k, 1] = (PG[k, 64:96, width:] + FR[k, 1].astype(F32)).astype(BF16)
        joint(k, 0).start()
        joint(k, 1).start()

    def add_y(k):
        for g in (0, 1):
            arrive(joint(k, g))
            arrive(direct(k, g))
        for g in (0, 1):
            total = PG[k, 96:128, g * width : (g + 1) * width] + (SR[k, g].astype(F32) + SR[k, 2 + g].astype(F32))
            YB[k, 0, g] = total[0:16]
            YB[k, 1, g] = total[16:32]
        cross_sum(k).start()

    def activate(k):
        arrive(cross_sum(k))
        gate = YB[k, xl, 0] + XR[k, 0]
        up = YB[k, xl, 1] + XR[k, 1]
        HB[k, c, y, xl] = (gate / (1 + jnp.exp(-gate)) * up).astype(BF16)
        cross_h(k, xl).start()

    def spread_y(k):
        arrive(cross_h(k, 1 - xl))
        for send in spreads(k):
            send.start()

    def to_twin(k):
        for piece in spread_in(k):
            arrive(piece)
        twin_h(k, c).start()

    def down(k):
        arrive(twin_h(k, 1 - c))

        if "d%d" % k == FIRST_DOWN:
            loads[3].wait()
            arrive(weight_in)

        @pl.loop(0, half // 256, unroll=True)
        def _(i):
            columns = pl.ds(pl.multiple_of(i * 256, 256), 256)
            own = jnp.dot(HB[k, 0].reshape(128, width), DW[0, :, columns], preferred_element_type=F32)
            total = own + jnp.dot(HB[k, 1].reshape(128, width), DW[1, :, columns], preferred_element_type=F32)
            PO[k, :, :, columns] = total.reshape(4, 32, 256)

        for part in (0, 1):
            XS[k, part] = PO[k, 2 * core_of(part) + 1 - xh].astype(BF16)
            halves(k, part).start()

    def send_part(k, part):
        arrive(halves(k, part))
        total = PO[k, 2 * core_of(part) + xh] + XD[k, part].astype(F32)
        if k == 0:
            FIN[part] = total
            if part == 1:
                own_copy.start()
        else:
            ZS[k, part] = total.astype(BF16)
            home(k, part).start()

    def send_z(k):
        send_part(k, 0)

    def send_other_z(k):
        send_part(k, 1)

    stages = dict(gate_up=gate_up, relay_y=relay_y, add_y=add_y, activate=activate, spread_y=spread_y, to_twin=to_twin, down=down, send_z=send_z, send_other_z=send_other_z)

    for step in ORDER:
        if step[0] == "h":
            with jax.named_scope(step):
                hop(int(step[1]), int(step[2]))
        else:
            with jax.named_scope(step + STAGES[step[0]]):
                stages[STAGES[step[0]]](int(step[1]))

    pair_in(0).wait_send()
    weight_out.wait_send()
    own_copy.wait_send()
    for part in (0, 1):
        for n in range(3):
            ring_down(n, part).wait_send()
            ring_up(n, part).wait_send()
    ring_down(3, 0).wait_send()
    ring_up(3, 1).wait_send()
    for k in range(SLABS):
        for g in (0, 1):
            twin_in(k, g, c).wait_send()
            far(k, g).wait_send()
            direct(k, g).wait_send()
            joint(k, g).wait_send()
        cross_sum(k).wait_send()
        cross_h(k, xl).wait_send()
        for send in spreads(k):
            send.wait_send()
        twin_h(k, c).wait_send()
        for part in (0, 1):
            halves(k, part).wait_send()

    arrive(own_copy)
    for k in range(1, SLABS):
        arrive(home(k, 0))
        arrive(home(k, 1))
    for part, (first, columns) in enumerate(((FIN.at[0], mine), (OTHER, other))):
        total = first[...]
        for k in range(1, SLABS):
            total += ZR[k, part].astype(F32)
        out[:, pl.ds(columns, half)] = total.astype(BF16)
    for k in range(1, SLABS):
        home(k, 0).wait_send()
        home(k, 1).wait_send()


def per_device(tokens, gate_weight, up_weight, down_weight):
    rows, depth = tokens.shape
    width = gate_weight.shape[1]
    half = down_weight.shape[1] // 2
    dma = pltpu.SemaphoreType.DMA
    return pl.pallas_call(
        kernel,
        out_shape=jax.ShapeDtypeStruct((rows, 2 * half), BF16),
        in_specs=[pl.BlockSpec(memory_space=pl.ANY)] * 4,
        out_specs=pl.BlockSpec(memory_space=pltpu.VMEM),
        scratch_shapes=[
            pltpu.VMEM((8, 4, rows, depth), BF16),
            pltpu.VMEM((depth, 2 * width), BF16),
            pltpu.VMEM((2, width, half), BF16),
            pltpu.VMEM((8, 128, 2 * width), F32),
            pltpu.VMEM((8, 2, 32, width), BF16),
            pltpu.VMEM((8, 2, 32, width), BF16),
            pltpu.VMEM((8, 4, 32, width), BF16),
            pltpu.VMEM((8, 4, 32, width), BF16),
            pltpu.VMEM((8, 2, 2, 16, width), F32),
            pltpu.VMEM((8, 2, 16, width), F32),
            pltpu.VMEM((8, 2, 4, 2, 16, width), BF16),
            pltpu.VMEM((8, 4, 32, half), F32),
            pltpu.VMEM((8, 2, 32, half), BF16),
            pltpu.VMEM((8, 2, 32, half), BF16),
            pltpu.VMEM((8, 2, 32, half), BF16),
            pltpu.VMEM((8, 2, 32, half), BF16),
            pltpu.VMEM((2, 32, half), F32),
            pltpu.VMEM((32, half), F32),
            dma((4,)),
            dma((TOTAL,)),
            dma((TOTAL,)),
        ],
        compiler_params=pltpu.CompilerParams(collective_id=0, has_side_effects=True, vmem_limit_bytes=67043328),
        name="block",
    )(tokens, gate_weight, up_weight, down_weight)


def solution(mesh):
    return jax.shard_map(
        per_device,
        mesh=mesh,
        in_specs=(P("dp", "mp"), P("mp", "dp"), P("mp", "dp"), P("dp", "mp")),
        out_specs=P("dp", "mp"),
        check_vma=False,
    )
```
